256 devices in a mesh: grp: 4 (over y, x), panel: 64 (over z, core).
Axes of the slice: x: 2, y: 2, z: 32, core: 2. Of those that a mesh axis runs over, the one named last changes fastest.
The devices are a block of a 4x8x32 slice.
Arguments:
- density: bfloat16 [8192, 16, 128], P(('grp', 'panel')), parts along dimension 0, may hold values from -6 to 6
- near_blocks: bfloat16 [8192, 8, 128, 128], P(('grp', 'panel')), parts along dimension 0, may hold values from -0.1875 to 0.1875
- neighbours: int32 [8192, 8], P(('grp', 'panel')), parts along dimension 0, may hold values from 0 to 2047, as said below
- counts: int32 [8192], P(('grp', 'panel')), parts along dimension 0, may hold values from 1 to 8, as said below
- coarse_map: int32 [8192], P(('grp', 'panel')), parts along dimension 0, may hold values from 0 to 127, as said below
- restrict: bfloat16 [8192, 128, 128], P(('grp', 'panel')), parts along dimension 0, may hold values from -0.125 to 0.125
- evaluate: bfloat16 [8192, 128, 128], P(('grp', 'panel')), parts along dimension 0, may hold values from -0.5 to 0.5
- coupling: float32 [512, 128], P(('grp', 'panel')), parts along dimension 0, as said below
Outputs:
- potential: bfloat16 [8192, 16, 128], P(('grp', 'panel')), parts along dimension 0
The draws below stay inside these ranges and needn't reach their ends.
There are 4 independent parts, one for each index of `grp`. The reference program is written for one: setup_inputs(seed, part) draws one part's arguments, and reference() takes and returns one part's arrays. A program takes and returns all parts, laid end to end along the dimension named above; each array names one. Nothing has to cross between parts.
Inputs may be any that keep to these rules, and one draw needn't show every extreme that they name: `neighbours`: slot 0 of block b is b itself; every entry lies within 16 blocks of b; in every draw some entry lies exactly 16 blocks below its block and some exactly 16 above. `counts`: every device holds blocks with all 8 slots live. `coarse_map`: block b's coarse cluster is one of the 2 clusters from (b // 32) * 2 on. `coupling`: the matrix is symmetric.
All inputs are finite; a program needn't handle non-finite values.
Results may differ from the reference program's by a relative error of at most 0.0042.
Values may be sent and summed in bfloat16 or wider, within the bound.
A program may use at most 64 MiB of HBM per device.

```python
import jax
import jax.numpy as jnp
from jax import lax

BLK = 128
RHS = 16
NB = 8
K = 128
COARSE_DEV = 2
BLK_DEV = 32
REACH = 16
NBLK = 2048
NCOARSE = 128


def near_tables(key):
    key_offsets = jax.random.fold_in(key, 11)
    key_counts = jax.random.fold_in(key, 12)
    block_rows = jnp.arange(NBLK).astype(jnp.int32)
    offsets = jax.random.randint(key_offsets, (NBLK, NB), -REACH, REACH + 1).astype(jnp.int32)
    within = block_rows % BLK_DEV
    first_row = within == 0
    last_row = within == BLK_DEV - 1
    second = jnp.where(first_row, -REACH, jnp.where(last_row, REACH, offsets[:, 1])).astype(jnp.int32)
    offsets = offsets.at[:, 1].set(second)
    offsets = offsets.at[:, 0].set(0)
    block_ids = jnp.clip(block_rows[:, None] + offsets, 0, NBLK - 1).astype(jnp.int32)
    live_counts = jax.random.randint(key_counts, (NBLK,), 1, NB + 1).astype(jnp.int32)
    live_counts = jnp.where(first_row | last_row, NB, live_counts).astype(jnp.int32)
    return (block_ids, live_counts)


def draw_neighbours(key, part):
    return near_tables(key)[0]


def draw_counts(key, part):
    return near_tables(key)[1]


def draw_coarse_map(key, part):
    block_rows = jnp.arange(NBLK).astype(jnp.int32)
    chosen = jax.random.randint(jax.random.fold_in(key, 21), (NBLK,), 0, COARSE_DEV).astype(jnp.int32)
    return (block_rows // BLK_DEV * COARSE_DEV + chosen).astype(jnp.int32)


def draw_coupling(key, part):
    inner = jax.random.fold_in(key, 31)
    base = jax.random.normal(inner, (NCOARSE, NCOARSE), jnp.float32)
    return ((base + base.T) * (0.7071 / NCOARSE ** 0.5)).astype(jnp.float32)


def block_scale(rng, extent, split, smallest, top_value):
    def one(axis_at, blocks):
        steps = jax.random.uniform(jax.random.fold_in(jax.random.fold_in(rng, 6), axis_at), (blocks,), jnp.float32, smallest / len(split), top_value / len(split))
        return jnp.repeat(jnp.exp(steps), extent[axis_at] // blocks).reshape((-1,) + (1,) * (len(extent) - axis_at - 1))

    loudness = one(*split[0])
    for cut in split[1:]:
        loudness = loudness * one(*cut)
    return loudness


def noise(stream_key, dims, scale, reach, split=(), held_as=jnp.bfloat16):
    factor_of = block_scale(stream_key, dims, split, -0.22, 0.18) if split else 1.0
    result = jax.random.normal(stream_key, dims, jnp.float32) * scale * factor_of
    return jnp.minimum(jnp.maximum(result, -reach), reach).astype(held_as)


def setup_inputs(seed: int = 0, part: int = 0) -> dict:
    key_of = jax.random.split(jax.random.key(seed), 9)
    own_keys = jax.random.split(jax.random.fold_in(key_of[8], part), 9)
    density = noise(own_keys[0], (NBLK, RHS, BLK), 1.0, 6.0, ((0, 64),))
    near_blocks = noise(own_keys[1], (NBLK, NB, BLK, BLK), (BLK * NB) ** -0.5, 0.1875, ((0, 64),))
    neighbours = draw_neighbours(jax.random.fold_in(jax.random.fold_in(key_of[8], part), 71), part)
    counts = draw_counts(jax.random.fold_in(jax.random.fold_in(key_of[8], part), 71), part)
    coarse_map = draw_coarse_map(jax.random.fold_in(jax.random.fold_in(key_of[8], part), 71), part)
    restrict = noise(own_keys[5], (NBLK, K, BLK), (BLK * BLK_DEV // COARSE_DEV) ** -0.5, 0.125, ((0, 64),))
    evaluate = noise(own_keys[6], (NBLK, K, BLK), K ** -0.5, 0.5, ((0, 64),))
    coupling = draw_coupling(jax.random.fold_in(jax.random.fold_in(key_of[8], part), 71), part)
    return {"density": density, "near_blocks": near_blocks, "neighbours": neighbours, "counts": counts, "coarse_map": coarse_map, "restrict": restrict, "evaluate": evaluate, "coupling": coupling}


def reference(density, near_blocks, neighbours, counts, coarse_map, restrict, evaluate, coupling):
    dens_full = density.astype(jnp.float32)

    def one_block(item):
        blocks, block_ids, live_count = item
        picked = dens_full[block_ids]
        live_slots = (jnp.arange(NB).astype(jnp.int32) < live_count)[:, None, None]
        picked = jnp.where(live_slots, picked, jnp.zeros_like(picked))
        return jnp.einsum('jpq,jrq->rp', blocks.astype(jnp.float32), picked)

    near_part = lax.map(one_block, (near_blocks, neighbours, counts))
    block_terms = jnp.einsum('bkp,brp->brk', restrict.astype(jnp.float32), dens_full)
    block_terms = block_terms.reshape(NBLK, RHS * K)
    moments = jax.ops.segment_sum(block_terms, coarse_map, num_segments=NCOARSE)
    local_exp = jnp.dot(coupling, moments, precision=lax.Precision.HIGHEST).astype(jnp.bfloat16)
    spread = local_exp[coarse_map].astype(jnp.float32).reshape(NBLK, RHS, K)
    far_part = jnp.einsum('bkp,brk->brp', evaluate.astype(jnp.float32), spread)
    return (near_part + far_part).astype(jnp.bfloat16)
```

```python
import functools

import jax
import jax.numpy as jnp
from jax import lax
from jax.experimental import pallas as pl
from jax.experimental.pallas import tpu as pltpu
from jax.sharding import PartitionSpec as P

GRP_PANEL = ("grp", "panel")
MESH = pl.DeviceIdType.MESH
PAIR = 2
URGENT = 2
NT = (((1,), (1,)), ((), ()))
NN = (((1,), (0,)), ((), ()))


def kernel(
    size,
    nbr_hbm,
    cnt_hbm,
    map_hbm,
    cpl_hbm,
    dens_hbm,
    near_hbm,
    res_hbm,
    eva_hbm,
    out_hbm,
    nbr,
    cnt,
    cmap,
    cpl,
    ext,
    near_v,
    res_v,
    eva_v,
    nearf,
    out_v,
    gath,
    own_m,
    cpl_v,
    acc,
    loc,
    loc_out,
    smem_sem,
    dens_sem,
    res_sem,
    near_sem,
    eva_sem,
    out_sem,
    cpl_sem,
    send_sem,
    chunk_sem,
    row_sem,
    halo_sem,
    loc_sem,
):
    chips = size // 2
    second = chips // 4
    relays = [r for r in range(PAIR)] + [second + r for r in range(PAIR)]
    count = len(relays)
    blocks, rhs, width = dens_hbm.shape
    slots = nbr_hbm.shape[0]
    reach = blocks // 2
    me = lax.axis_index("panel")
    chip = me // 2
    core = me % 2
    in_first = chip < PAIR
    in_second = jnp.logical_and(chip >= second, chip < second + PAIR)
    is_relay = jnp.logical_and(core == 1, jnp.logical_or(in_first, in_second))
    served = jnp.where(in_first, second // PAIR, (chips - second) // PAIR) * 2
    base = jnp.where(chip < second, 0, second)
    my_relay = (base + chip % PAIR) * 2 + 1
    place = (chip - base) // PAIR * 2 + core
    has_left = me > 0
    has_right = me < size - 1

    def remote(src, dst, ssem, rsem, device):
        return pltpu.make_async_remote_copy(
            src_ref=src,
            dst_ref=dst,
            send_sem=ssem,
            recv_sem=rsem,
            device_id={"panel": device},
            device_id_type=MESH,
        )

    barrier = pltpu.get_barrier_semaphore()

    def greet(device):
        pl.semaphore_signal(barrier, inc=1, device_id={"panel": device}, device_id_type=MESH)

    @pl.when(has_left)
    def _():
        greet(me - 1)

    @pl.when(has_right)
    def _():
        greet(me + 1)

    own = ext.at[pl.ds(reach, blocks)]
    load_dens = pltpu.make_async_copy(dens_hbm, own, dens_sem)
    load_dens.start()
    parts = 2
    per = blocks // parts
    load_res = []
    for i in range(parts):
        piece = pl.ds(i * per, per)
        cp = pltpu.make_async_copy(res_hbm.at[piece], res_v.at[piece], res_sem.at[i])
        cp.start()
        load_res.append(cp)
    small = [
        pltpu.make_async_copy(map_hbm, cmap, smem_sem.at[0]),
        pltpu.make_async_copy(nbr_hbm, nbr, smem_sem.at[1]),
        pltpu.make_async_copy(cnt_hbm, cnt, smem_sem.at[2]),
    ]
    for cp in small:
        cp.start()

    @pl.when(is_relay)
    def _():
        def body(k, carry):
            greet(lax.rem(me + k, size))
            return carry

        lax.fori_loop(1, size, body, 0)

    pieces = 4
    step = blocks // pieces
    load_near = []
    for i in range(pieces):
        piece = pl.ds(i * step, step)
        load_near.append(
            pltpu.make_async_copy(near_hbm.at[piece], near_v.at[piece], near_sem.at[i])
        )
    load_eva = pltpu.make_async_copy(eva_hbm, eva_v, eva_sem)

    for cp in small:
        cp.wait()
    load_dens.wait()
    total = jnp.zeros((2 * rhs, width), jnp.float32)
    zero = jnp.zeros((rhs, width), jnp.bfloat16)

    def add_moments(total, first, last):
        for b in range(first, last, 2):
            rows = []
            for c in range(2):
                rows.append(
                    jnp.concatenate(
                        [
                            jnp.where(cmap[b + k] == 2 * me + c, ext[reach + b + k], zero)
                            for k in range(2)
                        ],
                        axis=1,
                    )
                )
            lhs = jnp.concatenate(rows, axis=0)
            weights = jnp.concatenate([res_v[b], res_v[b + 1]], axis=1)
            total += lax.dot_general(lhs, weights, NT, preferred_element_type=jnp.float32)
        return total

    low_halo = ext.at[pl.ds(0, reach)]
    high_halo = ext.at[pl.ds(reach + blocks, reach)]
    first_rows = ext.at[pl.ds(reach, reach)]
    last_rows = ext.at[pl.ds(blocks, reach)]
    up = remote(last_rows, low_halo, send_sem.at[count + 1], halo_sem.at[0], me + 1)
    down = remote(first_rows, high_halo, send_sem.at[count + 2], halo_sem.at[1], me - 1)

    load_res[0].wait()
    for cp in load_near[:2]:
        cp.start()
    total = add_moments(total, 0, per)
    pl.semaphore_wait(
        barrier,
        count + has_left.astype(jnp.int32) + has_right.astype(jnp.int32) - is_relay.astype(jnp.int32),
    )
    pl.when(has_right)(up.start)
    pl.when(has_left)(down.start)
    load_res[1].wait()
    total = add_moments(total, per, blocks)
    own_m[...] = total.astype(jnp.bfloat16).reshape(2, rhs, width)
    for cp in load_near[2:]:
        cp.start()
    load_eva.start()

    def to_relay(r):
        device = 2 * relays[r] + 1
        cp = remote(own_m, gath.at[chip, core], send_sem.at[r], chunk_sem.at[chip, core], device)
        return me != device, cp

    def send_to(which):
        for r in which:
            other, cp = to_relay(r)
            pl.when(other)(cp.start)

    send_to(range(PAIR))
    rows_to = remote(cpl_hbm, cpl_v.at[place], send_sem.at[count], row_sem.at[place], my_relay)
    pl.when(jnp.logical_not(is_relay))(rows_to.start)

    def prepare():
        gath[chip, 1] = own_m[...]
        acc[...] = jnp.zeros(acc.shape, jnp.float32)
        mine = pltpu.make_async_copy(cpl_hbm, cpl_v.at[place], cpl_sem)
        mine.start()

        def row_body(k, carry):
            at = lax.rem(place + k, served)
            remote(cpl_v.at[at], cpl_v.at[at], send_sem.at[0], row_sem.at[at], me).wait_recv()
            return carry

        lax.fori_loop(1, served, row_body, 0)
        mine.wait()
        table = pltpu.make_async_copy(cpl_v, cpl, cpl_sem)
        table.start()
        table.wait()

    @pl.when(jnp.logical_and(is_relay, in_first))
    def _():
        prepare()

    for cp in load_near:
        cp.wait()

    @pl.when(has_left)
    def _():
        up.wait_recv()

    @pl.when(has_right)
    def _():
        down.wait_recv()

    @pl.when(jnp.logical_not(has_left))
    def _():
        ext[pl.ds(0, reach)] = jnp.zeros((reach, rhs, width), jnp.bfloat16)

    @pl.when(jnp.logical_not(has_right))
    def _():
        ext[pl.ds(reach + blocks, reach)] = jnp.zeros((reach, rhs, width), jnp.bfloat16)

    def near_block(b, carry):
        picked = []
        for j in range(slots):
            where = nbr[j, b] - (me * blocks - reach)
            where = jnp.minimum(jnp.maximum(where, 0), 2 * blocks - 1)
            picked.append(jnp.where(j < cnt[b], ext[where], zero))
        value = jnp.zeros((rhs, width), jnp.float32)
        for j in range(0, slots, 2):
            lhs = jnp.concatenate([picked[j], picked[j + 1]], axis=1)
            weights = jnp.concatenate([near_v[b, j], near_v[b, j + 1]], axis=1)
            value += lax.dot_general(lhs, weights, NT, preferred_element_type=jnp.float32)
        nearf[b] = value
        return carry

    lax.fori_loop(0, blocks, near_block, 0, unroll=2)
    send_to(range(PAIR, count))

    @pl.when(jnp.logical_and(is_relay, in_second))
    def _():
        prepare()

    for r in range(count):
        other, cp = to_relay(r)
        pl.when(other)(cp.wait_send)
    pl.when(jnp.logical_not(is_relay))(rows_to.wait_send)
    pl.when(has_right)(up.wait_send)
    pl.when(has_left)(down.wait_send)
    load_eva.wait()

    store = pltpu.make_async_copy(out_v, out_hbm, out_sem)

    def finish(one, two):
        for b in range(blocks):
            lhs = jnp.where(cmap[b] == 2 * me, one, two)
            far = lax.dot_general(lhs, eva_v[b], NN, preferred_element_type=jnp.float32)
            out_v[b] = (nearf[b] + far).astype(jnp.bfloat16)
        store.start()

    @pl.when(jnp.logical_not(is_relay))
    def _():
        remote(loc, loc, send_sem.at[0], loc_sem, me).wait_recv()
        finish(loc[0], loc[1])
        store.wait()

    @pl.when(is_relay)
    def _():
        def arrive(slot, which):
            ref = gath.at[slot, which]
            remote(ref, ref, send_sem.at[0], chunk_sem.at[slot, which], me).wait_recv()

        def moments_of(slot):
            return [gath[slot, q // 2, q % 2].astype(jnp.float32) for q in range(4)]

        def add(at, slot, moments):
            values = []
            for c in range(2):
                value = acc[at, c]
                for q in range(4):
                    value += cpl[at, c, 4 * slot + q] * moments[q]
                values.append(value)
            return values

        def take(slot):
            moments = moments_of(slot)

            def inner(k, carry):
                for at in [8 * k + n for n in range(8)]:
                    values = add(at, slot, moments)
                    acc[at, 0] = values[0]
                    acc[at, 1] = values[1]
                return carry

            lax.fori_loop(0, served // 8, inner, 0)

        arrive(chip, 0)
        take(chip)

        def both(d, carry):
            for sign in (1, -1):
                slot = lax.rem(chip + sign * d + chips, chips)
                for which in (0, 1):
                    arrive(slot, which)
                take(slot)
            return carry

        lax.fori_loop(1, chips // 2, both, 0)
        last = lax.rem(chip + chips // 2, chips)
        for which in (0, 1):
            arrive(last, which)
        moments = moments_of(last)

        def result(at):
            values = add(at, last, moments)
            for c in range(2):
                loc_out[at, c] = values[c].astype(jnp.bfloat16)

        def give(at):
            device = (at // 2 * PAIR + chip) * 2 + at % 2
            return remote(loc_out.at[at], loc, send_sem.at[count + 3 + at], loc_sem, device)

        result(0)
        give(0).start()
        result(1)
        for at in range(2, 2 * URGENT):
            result(at)
            give(at).start()
        finish(loc_out[1, 0], loc_out[1, 1])

        def rest(at, carry):
            result(at)
            give(at).start()
            return carry

        lax.fori_loop(2 * URGENT, served, rest, 0)
        store.wait()

        def sent(at, carry):
            give(at).wait_send()
            return carry

        give(0).wait_send()
        lax.fori_loop(2, served, sent, 0)


def shards(size, density, near_blocks, neighbours, counts, coarse_map, restrict, evaluate, coupling):
    blocks, rhs, width = density.shape
    slots = neighbours.shape[1]
    terms = restrict.shape[1]
    chips = size // 2
    served = 2 * (chips - chips // 4) // PAIR
    count = 2 * PAIR
    bf16, f32 = jnp.bfloat16, jnp.float32
    dma = pltpu.SemaphoreType.DMA
    anywhere = pl.BlockSpec(memory_space=pl.ANY)
    return pl.pallas_call(
        functools.partial(kernel, size),
        out_shape=jax.ShapeDtypeStruct(density.shape, bf16),
        in_specs=[anywhere] * 8,
        out_specs=anywhere,
        scratch_shapes=[
            pltpu.SMEM((slots, blocks), jnp.int32),
            pltpu.SMEM((blocks,), jnp.int32),
            pltpu.SMEM((blocks,), jnp.int32),
            pltpu.SMEM((served, 2, 2 * size), f32),
            pltpu.VMEM((2 * blocks, rhs, width), bf16),
            pltpu.VMEM(near_blocks.shape, bf16),
            pltpu.VMEM(restrict.shape, bf16),
            pltpu.VMEM(evaluate.shape, bf16),
            pltpu.VMEM((blocks, rhs, width), f32),
            pltpu.VMEM((blocks, rhs, width), bf16),
            pltpu.VMEM((chips, 2, 2, rhs, terms), bf16),
            pltpu.VMEM((2, rhs, terms), bf16),
            pltpu.VMEM((served, 2, 2 * size), f32),
            pltpu.VMEM((served, 2, rhs, terms), f32),
            pltpu.VMEM((2, rhs, terms), bf16),
            pltpu.VMEM((served, 2, rhs, terms), bf16),
            dma((3,)),
            dma,
            dma((2,)),
            dma((4,)),
            dma,
            dma,
            dma,
            dma((count + 3 + served,)),
            dma((chips, 2)),
            dma((served,)),
            dma((2,)),
            dma,
        ],
        compiler_params=pltpu.CompilerParams(
            collective_id=0, has_side_effects=True, vmem_limit_bytes=67043328
        ),
        name="operator",
    )(neighbours.T, counts, coarse_map, coupling, density, near_blocks, restrict, evaluate)


def solution(mesh):
    placed = (
        P(GRP_PANEL, None, None),
        P(GRP_PANEL, None, None, None),
        P(GRP_PANEL, None),
        P(GRP_PANEL),
        P(GRP_PANEL),
        P(GRP_PANEL, None, None),
        P(GRP_PANEL, None, None),
        P(GRP_PANEL, None),
    )
    return jax.shard_map(
        functools.partial(shards, mesh.shape["panel"]),
        mesh=mesh,
        in_specs=placed,
        out_specs=P(GRP_PANEL, None, None),
        check_vma=False,
    )
```

```python
import functools

import jax
import jax.numpy as jnp
from jax import lax
from jax.experimental import pallas as pl
from jax.experimental.pallas import tpu as pltpu
from jax.sharding import PartitionSpec as P

GRP_PANEL = ("grp", "panel")
MESH = pl.DeviceIdType.MESH
FIRST = 2
SECOND = 3
AT = 8
NT = (((1,), (1,)), ((), ()))
NN = (((1,), (0,)), ((), ()))


def kernel(
    size,
    nbr_hbm,
    cnt_hbm,
    map_hbm,
    cpl_hbm,
    dens_hbm,
    near_hbm,
    res_hbm,
    eva_hbm,
    out_hbm,
    nbr,
    cnt,
    cmap,
    cpl,
    ext,
    near_v,
    res_v,
    eva_v,
    nearf,
    out_v,
    gath,
    own_m,
    own_rows,
    cpl_v,
    acc,
    loc,
    loc_out,
    smem_sem,
    dens_sem,
    res_sem,
    near_sem,
    eva_sem,
    out_sem,
    cpl_sem,
    send_sem,
    chunk_sem,
    row_sem,
    halo_sem,
    loc_sem,
    result_sem,
):
    chips = size // 2
    second = chips // 4
    relays = [r for r in range(FIRST)] + [second + r for r in range(SECOND)]
    count = len(relays)
    blocks, rhs, width = dens_hbm.shape
    slots = nbr_hbm.shape[0]
    reach = blocks // 2
    me = lax.axis_index("panel")
    chip = me // 2
    core = me % 2
    in_first = chip < FIRST
    in_second = jnp.logical_and(chip >= second, chip < second + SECOND)
    is_relay = jnp.logical_and(core == 1, jnp.logical_or(in_first, in_second))
    first_served = 2 * (second // FIRST)
    second_served = 2 * ((chips - second) // SECOND)
    served = jnp.where(in_first, first_served, second_served)
    base = jnp.where(chip < second, 0, second)
    stride = jnp.where(chip < second, FIRST, SECOND)
    my_relay = (base + lax.rem(chip - base, stride)) * 2 + 1
    place = lax.div(chip - base, stride) * 2 + core
    has_left = me > 0
    has_right = me < size - 1

    def remote(src, dst, ssem, rsem, device):
        return pltpu.make_async_remote_copy(
            src_ref=src,
            dst_ref=dst,
            send_sem=ssem,
            recv_sem=rsem,
            device_id={"panel": device},
            device_id_type=MESH,
        )

    barrier = pltpu.get_barrier_semaphore()

    def greet(device):
        pl.semaphore_signal(barrier, inc=1, device_id={"panel": device}, device_id_type=MESH)

    @pl.when(has_left)
    def _():
        greet(me - 1)

    @pl.when(has_right)
    def _():
        greet(me + 1)

    own = ext.at[pl.ds(reach, blocks)]
    load_dens = pltpu.make_async_copy(dens_hbm, own, dens_sem)
    load_dens.start()
    parts = 2
    per = blocks // parts
    load_res = []
    for i in range(parts):
        piece = pl.ds(i * per, per)
        cp = pltpu.make_async_copy(res_hbm.at[piece], res_v.at[piece], res_sem.at[i])
        cp.start()
        load_res.append(cp)
    small = [
        pltpu.make_async_copy(map_hbm, cmap, smem_sem.at[0]),
        pltpu.make_async_copy(nbr_hbm, nbr, smem_sem.at[1]),
        pltpu.make_async_copy(cnt_hbm, cnt, smem_sem.at[2]),
        pltpu.make_async_copy(cpl_hbm, own_rows, smem_sem.at[3]),
    ]
    for cp in small:
        cp.start()

    @pl.when(is_relay)
    def _():
        def body(k, carry):
            greet(lax.rem(me + k, size))
            return carry

        lax.fori_loop(1, size, body, 0)

    pieces = 4
    step = blocks // pieces
    load_near = []
    for i in range(pieces):
        piece = pl.ds(i * step, step)
        load_near.append(
            pltpu.make_async_copy(near_hbm.at[piece], near_v.at[piece], near_sem)
        )
    load_eva = pltpu.make_async_copy(eva_hbm, eva_v, eva_sem)

    for cp in small:
        cp.wait()
    load_dens.wait()
    total = jnp.zeros((2 * rhs, width), jnp.float32)
    zero = jnp.zeros((rhs, width), jnp.bfloat16)

    def add_moments(total, first, last):
        rows = []
        for c in range(2):
            rows.append(
                jnp.concatenate(
                    [jnp.where(cmap[b] == 2 * me + c, ext[reach + b], zero) for b in range(first, last)],
                    axis=1,
                )
            )
        lhs = jnp.concatenate(rows, axis=0)
        weights = jnp.concatenate([res_v[b] for b in range(first, last)], axis=1)
        total += lax.dot_general(lhs, weights, NT, preferred_element_type=jnp.float32)
        return total

    low_halo = ext.at[pl.ds(0, reach)]
    high_halo = ext.at[pl.ds(reach + blocks, reach)]
    first_rows = ext.at[pl.ds(reach, reach)]
    last_rows = ext.at[pl.ds(blocks, reach)]
    up = remote(last_rows, low_halo, send_sem.at[count + 1], halo_sem.at[0], me + 1)
    down = remote(first_rows, high_halo, send_sem.at[count + 2], halo_sem.at[1], me - 1)

    load_res[0].wait()
    for cp in load_near[:2]:
        cp.start()
    total = add_moments(total, 0, per)
    load_res[1].wait()
    total = add_moments(total, per, blocks)
    own_m[...] = total.astype(jnp.bfloat16).reshape(2, rhs, width)
    for cp in load_near[2:]:
        cp.start()
    load_eva.start()

    def to_relay(r):
        device = 2 * relays[r] + 1
        ahead = lax.rem(chip - relays[r] + chips, chips)
        distance = jnp.minimum(ahead, chips - ahead)
        cp = remote(own_m, gath.at[me], send_sem.at[r], chunk_sem.at[distance], device)
        return me != device, cp

    def send_to(which):
        for r in which:
            other, cp = to_relay(r)
            pl.when(other)(cp.start)

    pl.semaphore_wait(
        barrier,
        count + has_left.astype(jnp.int32) + has_right.astype(jnp.int32) - is_relay.astype(jnp.int32),
    )
    rows_to = remote(own_rows, cpl_v.at[place], send_sem.at[count], row_sem, my_relay)
    pl.when(jnp.logical_not(is_relay))(rows_to.start)
    send_to(range(FIRST))
    pl.when(has_right)(up.start)
    pl.when(has_left)(down.start)
    send_to(range(FIRST, count))

    def prepare(n):
        gath[me] = own_m[...]
        acc[...] = jnp.zeros(acc.shape, jnp.float32)
        cpl_v[place] = own_rows[...]
        others = cpl_v.at[pl.ds(0, n - 1)]
        remote(others, others, send_sem.at[0], row_sem, me).wait_recv()
        table = pltpu.make_async_copy(cpl_v, cpl, cpl_sem)
        table.start()
        table.wait()

    @pl.when(jnp.logical_and(is_relay, in_first))
    def _():
        prepare(first_served)

    pltpu.make_async_copy(near_hbm, near_v, near_sem).wait()

    @pl.when(has_left)
    def _():
        up.wait_recv()

    @pl.when(has_right)
    def _():
        down.wait_recv()

    @pl.when(jnp.logical_not(has_left))
    def _():
        ext[pl.ds(0, reach)] = jnp.zeros((reach, rhs, width), jnp.bfloat16)

    @pl.when(jnp.logical_not(has_right))
    def _():
        ext[pl.ds(reach + blocks, reach)] = jnp.zeros((reach, rhs, width), jnp.bfloat16)

    def near_block(b, carry):
        picked = []
        for j in range(slots):
            where = nbr[j, b] - (me * blocks - reach)
            where = jnp.minimum(jnp.maximum(where, 0), 2 * blocks - 1)
            picked.append(jnp.where(j < cnt[b], ext[where], zero))
        value = jnp.zeros((rhs, width), jnp.float32)
        for j in range(0, slots, 2):
            lhs = jnp.concatenate([picked[j], picked[j + 1]], axis=1)
            weights = jnp.concatenate([near_v[b, j], near_v[b, j + 1]], axis=1)
            value += lax.dot_general(lhs, weights, NT, preferred_element_type=jnp.float32)
        nearf[b] = value
        return carry

    lax.fori_loop(0, blocks, near_block, 0, unroll=2)
    @pl.when(jnp.logical_and(is_relay, in_second))
    def _():
        prepare(second_served)

    load_eva.wait()


    def give(at):
        device = (at // 2 * stride + chip) * 2 + at % 2
        return remote(loc_out.at[at], loc, result_sem, loc_sem, device)

    last = lax.rem(chip + chips // 2, chips)

    def moments_of(slot):
        return [gath[2 * slot + q // 2, q % 2].astype(jnp.float32) for q in range(4)]

    def add(at, sources):
        values = []
        for c in range(2):
            value = acc[at, c]
            for slot, moments in sources:
                for q in range(4):
                    value += cpl[at, c, 4 * slot + q] * moments[q]
            values.append(value)
        return values

    def result(at, sources):
        values = add(at, sources)
        for c in range(2):
            loc_out[at, c] = values[c].astype(jnp.bfloat16)

    @pl.when(jnp.logical_not(is_relay))
    def _():
        remote(loc, loc, send_sem.at[0], loc_sem, me).wait_recv()

    @pl.when(is_relay)
    def _():
        def arrive(distance, number):
            ref = gath.at[pl.ds(0, number)]
            remote(ref, ref, send_sem.at[0], chunk_sem.at[distance], me).wait_recv()

        def take(slots_in):
            sources = [(slot, moments_of(slot)) for slot in slots_in]

            def inner(k, carry):
                for at in [AT * k + n for n in range(AT)]:
                    values = add(at, sources)
                    acc[at, 0] = values[0]
                    acc[at, 1] = values[1]
                return carry

            lax.fori_loop(0, served // AT, inner, 0)

        arrive(0, 1)
        take([chip])

        def both(d, carry):
            arrive(d, 4)
            take([lax.rem(chip + d, chips), lax.rem(chip - d + chips, chips)])
            return carry

        lax.fori_loop(1, chips // 2, both, 0)
        arrive(chips // 2, 2)
        sources = [(last, moments_of(last))]
        result(0, sources)
        give(0).start()
        result(1, sources)
        loc[...] = loc_out[1]

    one = loc[0]
    two = loc[1]
    stores = []
    for i in range(2):
        for b in range(i * per, (i + 1) * per):
            lhs = jnp.where(cmap[b] == 2 * me, one, two)
            far = lax.dot_general(lhs, eva_v[b], NN, preferred_element_type=jnp.float32)
            out_v[b] = (nearf[b] + far).astype(jnp.bfloat16)
        piece = pl.ds(i * per, per)
        stores.append(pltpu.make_async_copy(out_v.at[piece], out_hbm.at[piece], out_sem.at[i]))
        stores[i].start()

    @pl.when(is_relay)
    def _():
        sources = [(last, moments_of(last))]

        def rest(k, carry):
            for at in (2 * k, 2 * k + 1):
                result(at, sources)
                give(at).start()
            return carry

        lax.fori_loop(1, served // 2, rest, 0)

    for chosen, n in ((in_first, first_served), (in_second, second_served)):
        @pl.when(jnp.logical_and(is_relay, chosen))
        def _():
            ref = loc_out.at[pl.ds(0, n - 1)]
            remote(ref, ref, result_sem, loc_sem, me).wait_send()

    for r in range(count):
        other, cp = to_relay(r)
        pl.when(other)(cp.wait_send)
    pl.when(jnp.logical_not(is_relay))(rows_to.wait_send)
    pl.when(has_right)(up.wait_send)
    pl.when(has_left)(down.wait_send)
    for cp in stores:
        cp.wait()


def shards(size, density, near_blocks, neighbours, counts, coarse_map, restrict, evaluate, coupling):
    blocks, rhs, width = density.shape
    slots = neighbours.shape[1]
    terms = restrict.shape[1]
    chips = size // 2
    served = 2 * (chips - chips // 4) // SECOND
    count = FIRST + SECOND
    bf16, f32 = jnp.bfloat16, jnp.float32
    dma = pltpu.SemaphoreType.DMA
    anywhere = pl.BlockSpec(memory_space=pl.ANY)
    return pl.pallas_call(
        functools.partial(kernel, size),
        out_shape=jax.ShapeDtypeStruct(density.shape, bf16),
        in_specs=[anywhere] * 8,
        out_specs=anywhere,
        scratch_shapes=[
            pltpu.SMEM((slots, blocks), jnp.int32),
            pltpu.SMEM((blocks,), jnp.int32),
            pltpu.SMEM((blocks,), jnp.int32),
            pltpu.SMEM((served, 2, 2 * size), f32),
            pltpu.VMEM((2 * blocks, rhs, width), bf16),
            pltpu.VMEM(near_blocks.shape, bf16),
            pltpu.VMEM(restrict.shape, bf16),
            pltpu.VMEM(evaluate.shape, bf16),
            pltpu.VMEM((blocks, rhs, width), f32),
            pltpu.VMEM((blocks, rhs, width), bf16),
            pltpu.VMEM((size, 2, rhs, terms), bf16),
            pltpu.VMEM((2, rhs, terms), bf16),
            pltpu.VMEM((2, 2 * size), f32),
            pltpu.VMEM((served, 2, 2 * size), f32),
            pltpu.VMEM((served, 2, rhs, terms), f32),
            pltpu.VMEM((2, rhs, terms), bf16),
            pltpu.VMEM((served, 2, rhs, terms), bf16),
            dma((4,)),
            dma,
            dma((2,)),
            dma,
            dma,
            dma((2,)),
            dma,
            dma((count + 3,)),
            dma((chips // 2 + 1,)),
            dma,
            dma((2,)),
            dma,
            dma,
        ],
        compiler_params=pltpu.CompilerParams(
            collective_id=0, has_side_effects=True, vmem_limit_bytes=67043328
        ),
        name="operator",
    )(neighbours.T, counts, coarse_map, coupling, density, near_blocks, restrict, evaluate)


def solution(mesh):
    placed = (
        P(GRP_PANEL, None, None),
        P(GRP_PANEL, None, None, None),
        P(GRP_PANEL, None),
        P(GRP_PANEL),
        P(GRP_PANEL),
        P(GRP_PANEL, None, None),
        P(GRP_PANEL, None, None),
        P(GRP_PANEL, None),
    )
    return jax.shard_map(
        functools.partial(shards, mesh.shape["panel"]),
        mesh=mesh,
        in_specs=placed,
        out_specs=P(GRP_PANEL, None, None),
        check_vma=False,
    )
```

```python
import functools

import jax
import jax.numpy as jnp
from jax import lax
from jax.experimental import pallas as pl
from jax.experimental.pallas import tpu as pltpu
from jax.sharding import PartitionSpec as P

GRP_PANEL = ("grp", "panel")
MESH = pl.DeviceIdType.MESH
FIRST = 2
SECOND = 3
AT = 8
NT = (((1,), (1,)), ((), ()))
NN = (((1,), (0,)), ((), ()))


def kernel(
    size,
    nbr_hbm,
    cnt_hbm,
    map_hbm,
    cpl_hbm,
    dens_hbm,
    near_hbm,
    res_hbm,
    eva_hbm,
    out_hbm,
    nbr,
    cnt,
    cmap,
    cpl,
    ext,
    near_v,
    res_v,
    eva_v,
    nearf,
    out_v,
    gath,
    own_m,
    own_rows,
    cpl_v,
    acc,
    loc,
    loc_out,
    smem_sem,
    dens_sem,
    res_sem,
    near_sem,
    eva_sem,
    out_sem,
    cpl_sem,
    send_sem,
    chunk_sem,
    row_sem,
    halo_sem,
    loc_sem,
    result_sem,
):
    chips = size // 2
    second = chips // 4
    relays = [r for r in range(FIRST)] + [second + r for r in range(SECOND)]
    count = len(relays)
    blocks, rhs, width = dens_hbm.shape
    slots = nbr_hbm.shape[0]
    reach = blocks // 2
    me = lax.axis_index("panel")
    chip = me // 2
    core = me % 2
    in_first = chip < FIRST
    in_second = jnp.logical_and(chip >= second, chip < second + SECOND)
    is_relay = jnp.logical_and(core == 1, jnp.logical_or(in_first, in_second))
    first_served = 2 * (second // FIRST)
    second_served = 2 * ((chips - second) // SECOND)
    served = jnp.where(in_first, first_served, second_served)
    base = jnp.where(chip < second, 0, second)
    stride = jnp.where(chip < second, FIRST, SECOND)
    my_relay = (base + lax.rem(chip - base, stride)) * 2 + 1
    place = lax.div(chip - base, stride) * 2 + core
    has_left = me > 0
    has_right = me < size - 1

    def remote(src, dst, ssem, rsem, device):
        return pltpu.make_async_remote_copy(
            src_ref=src,
            dst_ref=dst,
            send_sem=ssem,
            recv_sem=rsem,
            device_id={"panel": device},
            device_id_type=MESH,
        )

    barrier = pltpu.get_barrier_semaphore()

    def greet(device):
        pl.semaphore_signal(barrier, inc=1, device_id={"panel": device}, device_id_type=MESH)

    @pl.when(has_left)
    def _():
        greet(me - 1)

    @pl.when(has_right)
    def _():
        greet(me + 1)

    own = ext.at[pl.ds(reach, blocks)]
    load_dens = pltpu.make_async_copy(dens_hbm, own, dens_sem)
    load_dens.start()
    parts = 2
    per = blocks // parts
    load_res = []
    for i in range(parts):
        piece = pl.ds(i * per, per)
        cp = pltpu.make_async_copy(res_hbm.at[piece], res_v.at[piece], res_sem.at[i])
        cp.start()
        load_res.append(cp)
    small = [
        pltpu.make_async_copy(map_hbm, cmap, smem_sem.at[0]),
        pltpu.make_async_copy(nbr_hbm, nbr, smem_sem.at[1]),
        pltpu.make_async_copy(cnt_hbm, cnt, smem_sem.at[2]),
        pltpu.make_async_copy(cpl_hbm, own_rows, smem_sem.at[3]),
    ]
    for cp in small:
        cp.start()

    @pl.when(is_relay)
    def _():
        def body(k, carry):
            greet(lax.rem(me + k, size))
            return carry

        lax.fori_loop(1, size, body, 0)

    pieces = 4
    step = blocks // pieces
    load_near = []
    for i in range(pieces):
        piece = pl.ds(i * step, step)
        load_near.append(
            pltpu.make_async_copy(near_hbm.at[piece], near_v.at[piece], near_sem)
        )
    load_eva = pltpu.make_async_copy(eva_hbm, eva_v, eva_sem)

    for cp in small:
        cp.wait()
    load_dens.wait()
    zero = jnp.zeros((rhs, width), jnp.bfloat16)

    def add_moments():
        sums = []
        quarter = blocks // 4
        for first in range(0, blocks, quarter):
            span = range(first, first + quarter)
            rows = []
            for c in range(2):
                rows.append(
                    jnp.concatenate(
                        [jnp.where(cmap[b] == 2 * me + c, ext[reach + b], zero) for b in span], axis=1
                    )
                )
            lhs = jnp.concatenate(rows, axis=0)
            weights = jnp.concatenate([res_v[b] for b in span], axis=1)
            sums.append(lax.dot_general(lhs, weights, NT, preferred_element_type=jnp.float32))
        return (sums[0] + sums[1]) + (sums[2] + sums[3])

    low_halo = ext.at[pl.ds(0, reach)]
    high_halo = ext.at[pl.ds(reach + blocks, reach)]
    first_rows = ext.at[pl.ds(reach, reach)]
    last_rows = ext.at[pl.ds(blocks, reach)]
    up = remote(last_rows, low_halo, send_sem.at[count + 1], halo_sem.at[0], me + 1)
    down = remote(first_rows, high_halo, send_sem.at[count + 2], halo_sem.at[1], me - 1)

    for cp in load_res:
        cp.wait()
    for cp in load_near[:2]:
        cp.start()
    total = add_moments()
    own_m[...] = total.astype(jnp.bfloat16).reshape(2, rhs, width)
    for cp in load_near[2:]:
        cp.start()
    load_eva.start()

    def to_relay(r):
        device = 2 * relays[r] + 1
        ahead = lax.rem(chip - relays[r] + chips, chips)
        distance = jnp.minimum(ahead, chips - ahead)
        cp = remote(own_m, gath.at[me], send_sem.at[r], chunk_sem.at[distance], device)
        return me != device, cp

    def send_to(which):
        for r in which:
            other, cp = to_relay(r)
            pl.when(other)(cp.start)

    pl.semaphore_wait(
        barrier,
        count + has_left.astype(jnp.int32) + has_right.astype(jnp.int32) - is_relay.astype(jnp.int32),
    )
    rows_to = remote(own_rows, cpl_v.at[place], send_sem.at[count], row_sem, my_relay)
    pl.when(jnp.logical_not(is_relay))(rows_to.start)
    send_to(range(FIRST))
    pl.when(has_right)(up.start)
    pl.when(has_left)(down.start)
    send_to(range(FIRST, count))

    def prepare(n):
        gath[me] = own_m[...]
        acc[...] = jnp.zeros(acc.shape, jnp.float32)
        cpl_v[place] = own_rows[...]
        others = cpl_v.at[pl.ds(0, n - 1)]
        remote(others, others, send_sem.at[0], row_sem, me).wait_recv()
        table = pltpu.make_async_copy(cpl_v, cpl, cpl_sem)
        table.start()
        table.wait()

    @pl.when(jnp.logical_and(is_relay, in_first))
    def _():
        prepare(first_served)

    pltpu.make_async_copy(near_hbm, near_v, near_sem).wait()

    @pl.when(has_left)
    def _():
        up.wait_recv()

    @pl.when(has_right)
    def _():
        down.wait_recv()

    @pl.when(jnp.logical_not(has_left))
    def _():
        ext[pl.ds(0, reach)] = jnp.zeros((reach, rhs, width), jnp.bfloat16)

    @pl.when(jnp.logical_not(has_right))
    def _():
        ext[pl.ds(reach + blocks, reach)] = jnp.zeros((reach, rhs, width), jnp.bfloat16)

    def near_block(b, carry):
        picked = []
        for j in range(slots):
            where = nbr[j, b] - (me * blocks - reach)
            where = jnp.minimum(jnp.maximum(where, 0), 2 * blocks - 1)
            picked.append(jnp.where(j < cnt[b], ext[where], zero))
        value = jnp.zeros((rhs, width), jnp.float32)
        for j in range(0, slots, 2):
            lhs = jnp.concatenate([picked[j], picked[j + 1]], axis=1)
            weights = jnp.concatenate([near_v[b, j], near_v[b, j + 1]], axis=1)
            value += lax.dot_general(lhs, weights, NT, preferred_element_type=jnp.float32)
        nearf[b] = value
        return carry

    lax.fori_loop(0, blocks, near_block, 0, unroll=2)
    @pl.when(jnp.logical_and(is_relay, in_second))
    def _():
        prepare(second_served)

    load_eva.wait()


    def give(at):
        device = (at // 2 * stride + chip) * 2 + at % 2
        return remote(loc_out.at[at], loc, result_sem, loc_sem, device)

    last = lax.rem(chip + chips // 2, chips)

    def moments_of(slot):
        return [gath[2 * slot + q // 2, q % 2].astype(jnp.float32) for q in range(4)]

    def add(at, sources):
        values = []
        for c in range(2):
            value = acc[at, c]
            for slot, moments in sources:
                for q in range(4):
                    value += cpl[at, c, 4 * slot + q] * moments[q]
            values.append(value)
        return values

    def result(at, sources):
        values = add(at, sources)
        for c in range(2):
            loc_out[at, c] = values[c].astype(jnp.bfloat16)

    @pl.when(jnp.logical_not(is_relay))
    def _():
        remote(loc, loc, send_sem.at[0], loc_sem, me).wait_recv()

    @pl.when(is_relay)
    def _():
        def arrive(distance, number):
            ref = gath.at[pl.ds(0, number)]
            remote(ref, ref, send_sem.at[0], chunk_sem.at[distance], me).wait_recv()

        def take(slots_in):
            sources = [(slot, moments_of(slot)) for slot in slots_in]

            def inner(k, carry):
                for at in [AT * k + n for n in range(AT)]:
                    values = add(at, sources)
                    acc[at, 0] = values[0]
                    acc[at, 1] = values[1]
                return carry

            lax.fori_loop(0, served // AT, inner, 0)

        arrive(0, 1)
        take([chip])

        def both(d, carry):
            arrive(d, 4)
            take([lax.rem(chip + d, chips), lax.rem(chip - d + chips, chips)])
            return carry

        lax.fori_loop(1, chips // 2, both, 0)
        arrive(chips // 2, 2)
        sources = [(last, moments_of(last))]
        result(0, sources)
        give(0).start()
        result(1, sources)
        loc[...] = loc_out[1]

        @pl.when(in_first)
        def _():
            for at in range(2, first_served):
                result(at, sources)
                give(at).start()

        @pl.when(in_second)
        def _():
            others = second_served // 2 - 1

            def rest(i, carry):
                k = 1 + lax.rem(i + others // 2, others)
                for at in (2 * k, 2 * k + 1):
                    result(at, sources)
                    give(at).start()
                return carry

            lax.fori_loop(0, others, rest, 0)

    one = loc[0]
    two = loc[1]
    stores = []
    for i in range(2):
        for b in range(i * per, (i + 1) * per):
            lhs = jnp.where(cmap[b] == 2 * me, one, two)
            far = lax.dot_general(lhs, eva_v[b], NN, preferred_element_type=jnp.float32)
            out_v[b] = (nearf[b] + far).astype(jnp.bfloat16)
        piece = pl.ds(i * per, per)
        stores.append(pltpu.make_async_copy(out_v.at[piece], out_hbm.at[piece], out_sem.at[i]))
        stores[i].start()

    for chosen, n in ((in_first, first_served), (in_second, second_served)):
        @pl.when(jnp.logical_and(is_relay, chosen))
        def _():
            ref = loc_out.at[pl.ds(0, n - 1)]
            remote(ref, ref, result_sem, loc_sem, me).wait_send()

    for r in range(count):
        other, cp = to_relay(r)
        pl.when(other)(cp.wait_send)
    pl.when(jnp.logical_not(is_relay))(rows_to.wait_send)
    pl.when(has_right)(up.wait_send)
    pl.when(has_left)(down.wait_send)
    for cp in stores:
        cp.wait()


def shards(size, density, near_blocks, neighbours, counts, coarse_map, restrict, evaluate, coupling):
    blocks, rhs, width = density.shape
    slots = neighbours.shape[1]
    terms = restrict.shape[1]
    chips = size // 2
    served = 2 * (chips - chips // 4) // SECOND
    count = FIRST + SECOND
    bf16, f32 = jnp.bfloat16, jnp.float32
    dma = pltpu.SemaphoreType.DMA
    anywhere = pl.BlockSpec(memory_space=pl.ANY)
    return pl.pallas_call(
        functools.partial(kernel, size),
        out_shape=jax.ShapeDtypeStruct(density.shape, bf16),
        in_specs=[anywhere] * 8,
        out_specs=anywhere,
        scratch_shapes=[
            pltpu.SMEM((slots, blocks), jnp.int32),
            pltpu.SMEM((blocks,), jnp.int32),
            pltpu.SMEM((blocks,), jnp.int32),
            pltpu.SMEM((served, 2, 2 * size), f32),
            pltpu.VMEM((2 * blocks, rhs, width), bf16),
            pltpu.VMEM(near_blocks.shape, bf16),
            pltpu.VMEM(restrict.shape, bf16),
            pltpu.VMEM(evaluate.shape, bf16),
            pltpu.VMEM((blocks, rhs, width), f32),
            pltpu.VMEM((blocks, rhs, width), bf16),
            pltpu.VMEM((size, 2, rhs, terms), bf16),
            pltpu.VMEM((2, rhs, terms), bf16),
            pltpu.VMEM((2, 2 * size), f32),
            pltpu.VMEM((served, 2, 2 * size), f32),
            pltpu.VMEM((served, 2, rhs, terms), f32),
            pltpu.VMEM((2, rhs, terms), bf16),
            pltpu.VMEM((served, 2, rhs, terms), bf16),
            dma((4,)),
            dma,
            dma((2,)),
            dma,
            dma,
            dma((2,)),
            dma,
            dma((count + 3,)),
            dma((chips // 2 + 1,)),
            dma,
            dma((2,)),
            dma,
            dma,
        ],
        compiler_params=pltpu.CompilerParams(
            collective_id=0, has_side_effects=True, vmem_limit_bytes=67043328
        ),
        name="operator",
    )(neighbours.T, counts, coarse_map, coupling, density, near_blocks, restrict, evaluate)


def solution(mesh):
    placed = (
        P(GRP_PANEL, None, None),
        P(GRP_PANEL, None, None, None),
        P(GRP_PANEL, None),
        P(GRP_PANEL),
        P(GRP_PANEL),
        P(GRP_PANEL, None, None),
        P(GRP_PANEL, None, None),
        P(GRP_PANEL, None),
    )
    return jax.shard_map(
        functools.partial(shards, mesh.shape["panel"]),
        mesh=mesh,
        in_specs=placed,
        out_specs=P(GRP_PANEL, None, None),
        check_vma=False,
    )
```
